32 devices in a mesh: dp: 4 (over z), ctx: 4 (over y, core), tp: 2 (over x).
Axes of the slice: x: 2, y: 2, z: 4, core: 2. Of those that a mesh axis runs over, the one named last changes fastest.
Arguments:
- queries: bfloat16 [4, 512, 4096], P('dp', 'ctx', 'tp'), may hold values from -8 to 8
- keys_text: bfloat16 [4, 512, 512], P('dp', 'ctx', 'tp'), may hold values from -8 to 8
- values_text: bfloat16 [4, 512, 512], P('dp', 'ctx', 'tp'), may hold values from -6 to 6
- patch_rows: bfloat16 [4, 4, 8, 2, 512], P('dp', 'ctx', None, None, 'tp'), may hold values from -6 to 6
- patch_owner: int32 [4, 4, 8, 1], P('dp', 'ctx'), may hold values from 0 to 3; in each aligned block of 8 rows (0 to 7, 8 to 15, ..., all dimensions but the last counted through in order) at most 4 rows name the same one
- patch_place: int32 [4, 4, 8], P('dp', 'ctx'), may hold values from 0 to 127
- value_head: bfloat16 [4096], P('tp'), may hold values from -0.75 to 0.75
Outputs:
- attention: bfloat16 [4, 512, 4096], P('dp', 'ctx', 'tp')
- value_out: float32 [4, 512], P('dp', 'ctx')
The draws below stay inside these ranges and needn't reach their ends.
Inputs may be any that keep to these rules, and one draw needn't show every extreme that they name: `patch_owner`: among the rows of one vision shard at most 4 name the same sequence, and exactly 4 do in some shards. `patch_place`: rows that share an owner, a ctx index and a position are all added there.
All inputs are finite; a program needn't handle non-finite values.
Results may differ from the reference program's by a relative error of at most 0.0079.
Values may be sent and summed in bfloat16 or wider, within the bound.
A program may use at most 64 MiB of HBM per device.

```python
import math
import jax
import jax.numpy as jnp
import numpy as np
from jax import lax

QHEADS = 32
KVHEADS = 4
HD = 128
TOK_DEV = 128
CAP = 4
LEN = 512
PATCH_DEV = 8
N_DP = 4
N_CTX = 4


def draw_queries(key, part):
    own_key = jax.random.fold_in(key, 11)
    drawn = jnp.clip(jax.random.normal(own_key, (N_DP, LEN, QHEADS * HD), jnp.float32), -8.0, 8.0)
    return drawn.astype(jnp.bfloat16)


def draw_keys_text(key, part):
    own_key = jax.random.fold_in(key, 13)
    drawn = jnp.clip(jax.random.normal(own_key, (N_DP, LEN, KVHEADS * HD), jnp.float32), -8.0, 8.0)
    return drawn.astype(jnp.bfloat16)


def plant(array, key, low, high):
    longest = array.shape.index(max(array.shape))
    spots = []
    for shift in (0, 1):
        where = [jax.random.randint(jax.random.fold_in(key, axis), (), 0, length) for axis, length in enumerate(array.shape)]
        where[longest] = (where[longest] + shift) % array.shape[longest]
        spots.append(tuple(where))
    return array.at[spots[0]].set(low).at[spots[1]].set(high)


def block_levels(rng, dims, pieces, smallest, top_value):
    def one(dim, parts):
        draws = jax.random.uniform(jax.random.fold_in(jax.random.fold_in(rng, 6), dim), (parts,), jnp.float32, smallest / len(pieces), top_value / len(pieces))
        return jnp.repeat(jnp.exp(draws), dims[dim] // parts).reshape((-1,) + (1,) * (len(dims) - dim - 1))

    gain = one(*pieces[0])
    for cut in pieces[1:]:
        gain = gain * one(*cut)
    return gain


def routed_block(key, own, number, rows, count, top, most, lean):
    order = jax.random.permutation(key, count)
    packed, ordinary = shares(count, rows * top, most, lean, True), shares(count, rows * top, most, lean, False)
    places = jnp.arange(count)

    def named(lengths, turn):
        used = int((lengths > 0).sum())
        fixed = max(1, used // 4)
        shifted = fixed + (places - fixed + turn * (used - fixed)) % max(1, count - fixed)
        return jnp.zeros((count,), jnp.int32).at[order[jnp.where(places < fixed, places, shifted)]].set(jnp.asarray(lengths, jnp.int32))

    lengths = jnp.where(number % 4 == 0, named(packed, number // 4), named(ordinary, number - number // 4 - 1))
    mixed = jax.random.permutation(jax.random.fold_in(own, 3), count)
    source_of, receiver = mixed[0:count // 2 * 2:2], mixed[1:count // 2 * 2:2]
    slack = jnp.minimum(lengths[source_of] - 1, most - lengths[receiver]) // 2
    slack = jnp.where((source_of == order[0]) | (receiver == order[0]) | (lengths[receiver] == 0), 0, jnp.maximum(slack, 0))
    shifted = jax.random.randint(jax.random.fold_in(own, 4), (count // 2,), 0, 1 << 20) % (slack + 1)
    lengths = lengths.at[source_of].add(-shifted).at[receiver].add(shifted)
    items = jnp.searchsorted(jnp.cumsum(lengths), jnp.arange(rows * top), side="right").astype(jnp.int32)
    listing = items.reshape(top, rows).T
    listing = listing[jax.random.permutation(jax.random.fold_in(own, 1), rows)]
    turn = jax.random.randint(jax.random.fold_in(own, 2), (rows, 1), 0, top)
    return jnp.take_along_axis(listing, (jnp.arange(top)[None, :] + turn) % top, axis=1)


def shares(amount, total, bound, lean, full):
    portions = [(1 << 20) // math.isqrt(grade ** lean) + 1 for grade in range(1, amount + 1)]
    largest = bound if full else min(bound, max(-(-total // amount), total * portions[0] // sum(portions)))
    least = 1 if total - largest >= amount - 1 else 0
    holding, surplus = [largest] + [least] * (amount - 1), total - largest - least * (amount - 1)
    while surplus > 0:
        movable = [i for i in range(1, amount) if holding[i] < largest] or [i for i in range(1, amount) if holding[i] < bound]
        mass, left = sum([portions[i] for i in movable]), surplus
        for i in movable:
            more = min(bound - holding[i], max(1, left * portions[i] // mass), surplus)
            holding[i] = holding[i] + more
            surplus = surplus - more
    return np.array(holding)


def gaussian(stream_key, extent, scale, reach, cuts=(), kind=jnp.bfloat16):
    gain = block_levels(stream_key, extent, cuts, -0.22, 0.18) if cuts else 1.0
    values = jax.random.normal(stream_key, extent, jnp.float32) * scale * gain
    return jnp.minimum(jnp.maximum(values, -reach), reach).astype(kind)


def setup_inputs(seed: int = 0) -> dict:
    key_list = jax.random.split(jax.random.key(seed), 8)
    queries = draw_queries(jax.random.fold_in(key_list[7], 71), 0)
    keys_text = draw_keys_text(jax.random.fold_in(key_list[7], 71), 0)
    values_text = gaussian(key_list[2], (N_DP, LEN, KVHEADS * HD), 1.0, 6.0, ((0, 4), (1, 4), (2, 2)))
    patch_rows = gaussian(key_list[3], (N_DP, N_CTX, PATCH_DEV, 2, KVHEADS * HD), 1.0, 6.0, ((0, 4), (1, 4), (4, 2)))
    patch_owner_keys = jax.random.split(jax.random.fold_in(key_list[4], 1), N_DP * N_CTX * PATCH_DEV // PATCH_DEV)
    patch_owner_turns = jax.random.permutation(jax.random.fold_in(key_list[4], 3), N_DP * N_CTX * PATCH_DEV // PATCH_DEV)
    patch_owner = jax.vmap(lambda own, number: routed_block(jax.random.fold_in(key_list[4], 2), own, number, PATCH_DEV, N_DP, 1, CAP, 2))(patch_owner_keys, patch_owner_turns).reshape((N_DP, N_CTX, PATCH_DEV, 1))
    patch_place = plant(jax.random.randint(key_list[5], (N_DP, N_CTX, PATCH_DEV), 0, TOK_DEV), jax.random.fold_in(key_list[5], 1), 0, TOK_DEV - 1).astype(jnp.int32)
    value_head = gaussian(key_list[6], (QHEADS * HD,), 64 ** -0.5, 0.75, ((0, 2),))
    return dict(queries=queries, keys_text=keys_text, values_text=values_text, patch_rows=patch_rows, patch_owner=patch_owner, patch_place=patch_place, value_head=value_head)


def attend(queries_seq, keys_seq, values_seq):
    length = queries_seq.shape[0]
    groups = keys_seq.shape[1] // HD
    group_size = queries_seq.shape[1] // keys_seq.shape[1]
    score_scale = HD ** -0.5
    query_split = queries_seq.reshape(length, groups, group_size, HD).astype(jnp.float32)
    key_split = keys_seq.reshape(length, groups, HD).astype(jnp.float32)
    value_split = values_seq.reshape(length, groups, HD).astype(jnp.float32)
    block_rows = 512 if length % 512 == 0 else length
    results = []
    for lower in range(0, length, block_rows):
        upper = lower + block_rows
        scores = jnp.einsum("tgrd,sgd->tgrs", query_split[lower:upper], key_split[:upper]) * score_scale
        allowed = jnp.arange(upper, dtype=jnp.int32)[None, :] <= (lower + jnp.arange(block_rows, dtype=jnp.int32))[:, None]
        allowed = allowed[:, None, None, :]
        scores = jnp.where(allowed, scores, -1e30)
        row_max = jnp.max(scores, axis=-1)
        weights = jnp.where(allowed, jnp.exp(scores - row_max[..., None]), 0.0)
        denominator = jnp.sum(weights, axis=-1)
        rounded = weights.astype(jnp.bfloat16).astype(jnp.float32)
        numerator = jnp.einsum("tgrs,sgd->tgrd", rounded, value_split[:upper])
        mixed = numerator / denominator[..., None]
        results.append(mixed.reshape(block_rows, queries_seq.shape[1]).astype(jnp.bfloat16))
    return jnp.concatenate(results, axis=0)


def reference(queries, keys_text, values_text, patch_rows, patch_owner, patch_place, value_head):
    kv_width = keys_text.shape[2]
    owner_seq = patch_owner[..., 0]
    row_place = jnp.arange(N_CTX, dtype=jnp.int32)[None, :, None] * TOK_DEV + patch_place
    flat_index = (owner_seq * LEN + row_place).reshape(-1).astype(jnp.int32)
    key_add = patch_rows[:, :, :, 0, :].reshape(-1, kv_width).astype(jnp.float32)
    value_add = patch_rows[:, :, :, 1, :].reshape(-1, kv_width).astype(jnp.float32)
    merged_keys = keys_text.reshape(-1, kv_width).astype(jnp.float32).at[flat_index].add(key_add)
    merged_values = values_text.reshape(-1, kv_width).astype(jnp.float32).at[flat_index].add(value_add)
    merged_keys = merged_keys.astype(jnp.bfloat16).reshape(N_DP, LEN, kv_width)
    merged_values = merged_values.astype(jnp.bfloat16).reshape(N_DP, LEN, kv_width)

    def per_sequence(triple):
        return attend(triple[0], triple[1], triple[2])

    attention = lax.map(per_sequence, (queries, merged_keys, merged_values))
    value_out = jnp.dot(attention.reshape(-1, attention.shape[2]), value_head, preferred_element_type=jnp.float32)
    return attention, value_out.reshape(N_DP, LEN)
```

```python
import functools
import math

import jax
import jax.numpy as jnp
from jax import lax
from jax.experimental import pallas as pl
from jax.experimental.pallas import tpu as pltpu
from jax.sharding import PartitionSpec as P

HD = 128
CAP = 4
SLOT_BYTES = 8 * 2**20
MESH = pl.DeviceIdType.MESH


def attend_block(
    carried, query_split, query_place, block_keys, block_values, key_place, score_scale
):
    running_max, denominator, numerator = carried
    scores = (
        jnp.einsum("tgrd,sgd->tgrs", query_split, block_keys, preferred_element_type=jnp.float32)
        * score_scale
    )
    allowed = (key_place[None, :] <= query_place[:, None])[:, None, None, :]
    scores = jnp.where(allowed, scores, -1e30)
    new_max = jnp.maximum(running_max, jnp.max(scores, axis=-1))
    weights = jnp.where(allowed, jnp.exp(scores - new_max[..., None]), 0.0)
    shrink = jnp.exp(running_max - new_max)
    denominator = denominator * shrink + jnp.sum(weights, axis=-1)
    numerator = numerator * shrink[..., None] + jnp.einsum(
        "tgrs,sgd->tgrd",
        weights.astype(jnp.bfloat16),
        block_values,
        preferred_element_type=jnp.float32,
    )
    return (new_max, denominator, numerator)


def unchanged(carried):
    return carried


def collective_body(queries, keys_text, values_text, patch_rows, patch_owner, patch_place, value_head):
    token_count = queries.shape[1]
    kv_width = keys_text.shape[2]
    groups = kv_width // HD
    head_count = queries.shape[2] // HD
    group_size = head_count // groups
    score_scale = HD ** (-0.5)
    dp_count = lax.axis_size("dp")
    slot_count = dp_count * CAP
    owner_seq = patch_owner[0, 0, :, 0]
    places = patch_place[0, 0]
    owner_hits = (owner_seq[:, None] == jnp.arange(dp_count, dtype=jnp.int32)[None, :]).astype(
        jnp.int32
    )
    before = jnp.cumsum(owner_hits, axis=0) - owner_hits
    slot_rank = jnp.sum(before * owner_hits, axis=1)
    target = owner_seq * CAP + slot_rank
    select = (jnp.arange(slot_count, dtype=jnp.int32)[:, None] == target[None, :]).astype(jnp.int32)
    row_data = patch_rows[0, 0].reshape(places.shape[0], 2 * kv_width)
    packed = jnp.dot(
        select.astype(jnp.bfloat16), row_data, preferred_element_type=jnp.float32
    ).astype(jnp.bfloat16)
    filled = jnp.sum(select, axis=1)
    slot_place = jnp.sum(select * places[None, :], axis=1) + (1 - filled) * token_count
    packed = packed.reshape(slot_count, 2, kv_width)
    arrived, arrived_place = (
        lax.all_to_all(packed, "dp", split_axis=0, concat_axis=0, tiled=True),
        lax.all_to_all(slot_place, "dp", split_axis=0, concat_axis=0, tiled=True),
    )
    landing = (jnp.arange(token_count, dtype=jnp.int32)[:, None] == arrived_place[None, :]).astype(
        jnp.bfloat16
    )
    arrivals = jnp.dot(
        landing, arrived.reshape(slot_count, 2 * kv_width), preferred_element_type=jnp.float32
    )
    merged_keys = (keys_text[0].astype(jnp.float32) + arrivals[:, :kv_width]).astype(jnp.bfloat16)
    merged_values = (values_text[0].astype(jnp.float32) + arrivals[:, kv_width:]).astype(
        jnp.bfloat16
    )
    query_split = queries[0].reshape(token_count, groups, group_size, HD)
    first_row = lax.axis_index("ctx") * token_count
    query_place = first_row + jnp.arange(token_count, dtype=jnp.int32)
    initial = (
        jnp.full((token_count, groups, group_size), -1e30, jnp.float32),
        jnp.zeros((token_count, groups, group_size), jnp.float32),
        jnp.zeros((token_count, groups, group_size, HD), jnp.float32),
    )
    carried = initial
    start_row = jnp.int32(0)
    piece_keys = lax.all_gather(merged_keys, "ctx", axis=0, tiled=True)
    piece_values = lax.all_gather(merged_values, "ctx", axis=0, tiled=True)
    piece_rows = piece_keys.shape[0]
    block_rows = min(512, piece_rows)
    for lower in range(0, piece_rows, block_rows):
        upper = min(lower + block_rows, piece_rows)
        block_keys = piece_keys[lower:upper].reshape(upper - lower, groups, HD)
        block_values = piece_values[lower:upper].reshape(upper - lower, groups, HD)
        key_place = start_row + lower + jnp.arange(upper - lower, dtype=jnp.int32)

        def update(state_in):
            return attend_block(
                state_in, query_split, query_place, block_keys, block_values, key_place, score_scale
            )

        carried = lax.cond(
            start_row + lower <= first_row + token_count - 1, update, unchanged, carried
        )
    running_max, denominator, numerator = carried
    attention = (
        (numerator / denominator[..., None])
        .reshape(token_count, head_count * HD)
        .astype(jnp.bfloat16)
    )
    partial_value = jnp.dot(attention, value_head, preferred_element_type=jnp.float32)
    value_out = lax.psum(partial_value, "tp")
    return (attention[None], value_out[None])


def fused_kernel(
    dp_count,
    ctx_count,
    tp_count,
    code_ref,
    rows_ref,
    keys_ref,
    values_ref,
    probe_ref,
    queries_hbm,
    out_ref,
    value_ref,
    queries,
    text,
    rows_in,
    code_in,
    merged_keys,
    merged_values,
    probe,
    partial,
    partial_in,
    query_sem,
    local_sem,
    text_send,
    text_recv,
    relay_send,
    patch_send,
    patch_recv,
    value_send,
    value_recv,
):
    d, c, t = lax.axis_index("dp"), lax.axis_index("ctx"), lax.axis_index("tp")
    token_count, kv_width = keys_ref.shape
    groups = kv_width // HD
    heads = queries.shape[1] // HD
    group_size = heads // groups
    paired = ctx_count % 2 == 0
    side = lax.rem(c, 2)
    partner = c + 1 - 2 * side

    load_queries = pltpu.make_async_copy(queries_hbm, queries, query_sem)
    load_queries.start()
    own_rows = pltpu.make_async_copy(rows_ref, rows_in.at[c, d], local_sem.at[0])
    own_code = pltpu.make_async_copy(code_ref, code_in.at[c, d], local_sem.at[1])
    own_rows.start()
    own_code.start()

    barrier = pltpu.get_barrier_semaphore()
    for k in range(dp_count):
        for m in range(ctx_count):
            if k or m:
                pl.semaphore_signal(
                    barrier,
                    inc=1,
                    device_id=(lax.rem(d + k, dp_count), lax.rem(c + m, ctx_count), t),
                    device_id_type=MESH,
                )
    for k in range(1, tp_count):
        pl.semaphore_signal(
            barrier, inc=1, device_id=(d, c, lax.rem(t + k, tp_count)), device_id_type=MESH
        )
    pl.semaphore_wait(barrier, dp_count * ctx_count - 1 + tp_count - 1)

    def patch_copies(k, later):
        there = lax.rem(d + k, dp_count)
        return [
            pltpu.make_async_remote_copy(
                src_ref=src,
                dst_ref=dst.at[c, d],
                send_sem=patch_send.at[later, k, kind],
                recv_sem=patch_recv.at[c, d, kind],
                device_id=(there, later, t),
                device_id_type=MESH,
            )
            for kind, (src, dst) in enumerate(((rows_ref, rows_in), (code_ref, code_in)))
        ]

    def text_copies(later):
        return [
            pltpu.make_async_remote_copy(
                src_ref=src,
                dst_ref=text.at[c, kind],
                send_sem=text_send.at[later, kind],
                recv_sem=text_recv.at[c, kind],
                device_id=(d, later, t),
                device_id_type=MESH,
            )
            for kind, src in enumerate((keys_ref, values_ref))
        ]

    def relay_copies(block):
        return [
            pltpu.make_async_remote_copy(
                src_ref=text.at[block, kind],
                dst_ref=text.at[block, kind],
                send_sem=relay_send.at[block, kind],
                recv_sem=text_recv.at[block, kind],
                device_id=(d, partner, t),
                device_id_type=MESH,
            )
            for kind in range(2)
        ]

    def sends_text(later):
        if not paired:
            return c < later
        return (c < later) & ((side == later % 2) | (partner == later))

    def for_patches(act):
        for k in range(dp_count):
            for later in range(ctx_count):
                reached = (c < later) if k == 0 else (c <= later)

                @pl.when(reached)
                def _():
                    for copy in patch_copies(k, later):
                        act(copy)

    def for_text(act):
        for later in range(1, ctx_count):

            @pl.when(sends_text(later))
            def _():
                for copy in text_copies(later):
                    act(copy)

    for_patches(lambda copy: copy.start())
    for_text(lambda copy: copy.start())

    probe[...] = probe_ref[...].astype(jnp.float32)
    own_rows.wait()
    own_code.wait()

    def wait_text(block):
        for copy in relay_copies(block):
            copy.wait_recv()

    def wait_patches(block, first):
        for k in range(first, dp_count):
            there = lax.rem(d + k, dp_count)
            for kind, (src, dst) in enumerate(((rows_ref, rows_in), (code_ref, code_in))):
                pltpu.make_async_remote_copy(
                    src_ref=src,
                    dst_ref=dst.at[block, there],
                    send_sem=patch_send.at[0, k, kind],
                    recv_sem=patch_recv.at[block, there, kind],
                    device_id=(there, c, t),
                    device_id_type=MESH,
                ).wait_recv()

    def merge(block, block_keys, block_values):
        slots = dp_count * rows_ref.shape[0]
        code = code_in[block].reshape(slots, 1)
        rows = rows_in[block].astype(jnp.float32).reshape(slots, 2 * kv_width)
        spots = d * token_count + lax.broadcasted_iota(jnp.int32, (slots, token_count), 1)
        landing = jnp.where(code == spots, 1.0, 0.0).astype(jnp.bfloat16)
        arrivals = lax.dot_general(
            landing,
            rows.astype(jnp.bfloat16),
            (((0,), (0,)), ((), ())),
            preferred_element_type=jnp.float32,
        )
        span = pl.ds(block * token_count, token_count)
        merged_keys[span, :] = (
            block_keys.astype(jnp.float32) + arrivals[:, :kv_width]
        ).astype(jnp.bfloat16)
        merged_values[span, :] = (
            block_values.astype(jnp.float32) + arrivals[:, kv_width:]
        ).astype(jnp.bfloat16)

    if paired:
        for block in range(ctx_count - 2):

            @pl.when((block < c) & (side == block % 2))
            def _():
                wait_text(block)

                @pl.when(block < c - side)
                def _():
                    for copy in relay_copies(block):
                        copy.start()

    for block in range(ctx_count):

        @pl.when(block == c)
        def _():
            wait_patches(block, 1)
            merge(block, keys_ref[...], values_ref[...])

        @pl.when(block < c)
        def _():
            wait_patches(block, 0)
            if paired:

                @pl.when(side != block % 2)
                def _():
                    wait_text(block)

            else:
                wait_text(block)
            merge(block, text[block, 0], text[block, 1])

    load_queries.wait()
    score_scale = HD ** (-0.5) * math.log2(math.e)

    def attend(last):
        length = (last + 1) * token_count
        row = lax.broadcasted_iota(jnp.int32, (token_count, token_count), 0)
        col = lax.broadcasted_iota(jnp.int32, (token_count, token_count), 1)
        allowed = col <= row
        unroll = math.gcd(group_size, 4)

        def step(number, total):
            first = number * unroll
            lane = pl.multiple_of((first // group_size) * HD, HD)
            block_keys = merged_keys[0:length, pl.ds(lane, HD)]
            block_values = merged_values[0:length, pl.ds(lane, HD)]
            for extra in range(unroll):
                head = first + extra
                place = pl.ds(pl.multiple_of(head * HD, HD), HD)
                scores = lax.dot_general(
                    queries[:, place],
                    block_keys,
                    (((1,), (1,)), ((), ())),
                    preferred_element_type=jnp.float32,
                )
                parts = [
                    scores[:, j * token_count : (j + 1) * token_count] for j in range(last + 1)
                ]
                parts[last] = jnp.where(allowed, parts[last], -1e30)
                top = functools.reduce(jnp.maximum, parts)
                top = jnp.max(top, axis=1, keepdims=True)
                weights = [jnp.exp2((part - top) * score_scale) for part in parts]
                denominator = jnp.sum(
                    functools.reduce(jnp.add, weights), axis=1, keepdims=True
                )
                rounded = jnp.concatenate([w.astype(jnp.bfloat16) for w in weights], axis=1)
                numerator = jnp.dot(rounded, block_values, preferred_element_type=jnp.float32)
                result = (numerator * (1.0 / denominator)).astype(jnp.bfloat16)
                out_ref[:, place] = result
                total = total + result.astype(jnp.float32) * probe[pl.ds(head, 1), :]
            return total

        total = lax.fori_loop(
            0, heads // unroll, step, jnp.zeros((token_count, HD), jnp.float32)
        )
        partial[...] = jnp.sum(jnp.transpose(total), axis=0, keepdims=True)

    for last in range(ctx_count):

        @pl.when(c == last)
        def _():
            attend(last)

    value_copies = [
        pltpu.make_async_remote_copy(
            src_ref=partial,
            dst_ref=partial_in.at[k - 1],
            send_sem=value_send.at[k - 1],
            recv_sem=value_recv.at[k - 1],
            device_id=(d, c, lax.rem(t + k, tp_count)),
            device_id_type=MESH,
        )
        for k in range(1, tp_count)
    ]
    for copy in value_copies:
        copy.start()
    for_patches(lambda copy: copy.wait_send())
    for_text(lambda copy: copy.wait_send())
    if paired:
        for block in range(ctx_count - 2):

            @pl.when((block < c - side) & (side == block % 2))
            def _():
                for copy in relay_copies(block):
                    copy.wait_send()

    for copy in value_copies:
        copy.wait()
    whole = partial[...]
    for k in range(1, tp_count):
        whole = whole + partial_in[k - 1]
    value_ref[...] = whole


def fused_body(sizes, queries, keys_text, values_text, patch_rows, patch_owner, patch_place, value_head):
    dp_count, ctx_count, tp_count = sizes
    _, token_count, query_width = queries.shape
    kv_width = keys_text.shape[2]
    row_count = patch_rows.shape[2]
    heads = query_width // HD
    code = patch_owner[0, 0] * token_count + patch_place[0, 0][:, None]
    rows = patch_rows[0, 0].reshape(row_count, 2 * kv_width)
    dma = pltpu.SemaphoreType.DMA
    vmem = pl.BlockSpec(memory_space=pltpu.VMEM)
    attention, value_out = pl.pallas_call(
        functools.partial(fused_kernel, dp_count, ctx_count, tp_count),
        out_shape=(
            jax.ShapeDtypeStruct((token_count, query_width), jnp.bfloat16),
            jax.ShapeDtypeStruct((1, token_count), jnp.float32),
        ),
        in_specs=[vmem] * 5 + [pl.BlockSpec(memory_space=pl.ANY)],
        out_specs=(vmem, vmem),
        scratch_shapes=[
            pltpu.VMEM((token_count, query_width), jnp.bfloat16),
            pltpu.VMEM((ctx_count, 2, token_count, kv_width), jnp.bfloat16),
            pltpu.VMEM((ctx_count, dp_count, row_count, 2 * kv_width), jnp.bfloat16),
            pltpu.VMEM((ctx_count, dp_count, row_count, 1), jnp.int32),
            pltpu.VMEM((ctx_count * token_count, kv_width), jnp.bfloat16),
            pltpu.VMEM((ctx_count * token_count, kv_width), jnp.bfloat16),
            pltpu.VMEM((heads, HD), jnp.float32),
            pltpu.VMEM((1, token_count), jnp.float32),
            pltpu.VMEM((max(tp_count - 1, 1), 1, token_count), jnp.float32),
            dma,
            dma((2,)),
            dma((ctx_count, 2)),
            dma((ctx_count, 2)),
            dma((ctx_count, 2)),
            dma((ctx_count, dp_count, 2)),
            dma((ctx_count, dp_count, 2)),
            dma((max(tp_count - 1, 1),)),
            dma((max(tp_count - 1, 1),)),
        ],
        compiler_params=pltpu.CompilerParams(
            collective_id=0, has_side_effects=True, vmem_limit_bytes=48 * 2**20
        ),
        name="merged_attention",
    )(code, rows, keys_text[0], values_text[0], value_head.reshape(heads, HD), queries[0])
    return (attention[None], value_out)


def body(sizes, queries, keys_text, values_text, patch_rows, patch_owner, patch_place, value_head):
    dp_count, ctx_count, _ = sizes
    arriving = dp_count * ctx_count * patch_rows.size * patch_rows.dtype.itemsize
    arrays = (queries, keys_text, values_text, patch_rows, patch_owner, patch_place, value_head)
    if arriving > SLOT_BYTES:
        return collective_body(*arrays)
    return fused_body(sizes, *arrays)


def solution(mesh):
    in_specs = (
        P("dp", "ctx", "tp"),
        P("dp", "ctx", "tp"),
        P("dp", "ctx", "tp"),
        P("dp", "ctx", None, None, "tp"),
        P("dp", "ctx", None, None),
        P("dp", "ctx", None),
        P("tp"),
    )
    out_specs = (P("dp", "ctx", "tp"), P("dp", "ctx"))
    sizes = tuple(mesh.shape[axis] for axis in ("dp", "ctx", "tp"))
    return jax.shard_map(
        functools.partial(body, sizes),
        mesh=mesh,
        in_specs=in_specs,
        out_specs=out_specs,
        check_vma=False,
    )
```

```python
import functools
import math

import jax
import jax.numpy as jnp
from jax import lax
from jax.experimental import pallas as pl
from jax.experimental.pallas import tpu as pltpu
from jax.sharding import PartitionSpec as P

HD = 128
CAP = 4
SLOT_BYTES = 8 * 2**20
MESH = pl.DeviceIdType.MESH


def attend_block(
    carried, query_split, query_place, block_keys, block_values, key_place, score_scale
):
    running_max, denominator, numerator = carried
    scores = (
        jnp.einsum("tgrd,sgd->tgrs", query_split, block_keys, preferred_element_type=jnp.float32)
        * score_scale
    )
    allowed = (key_place[None, :] <= query_place[:, None])[:, None, None, :]
    scores = jnp.where(allowed, scores, -1e30)
    new_max = jnp.maximum(running_max, jnp.max(scores, axis=-1))
    weights = jnp.where(allowed, jnp.exp(scores - new_max[..., None]), 0.0)
    shrink = jnp.exp(running_max - new_max)
    denominator = denominator * shrink + jnp.sum(weights, axis=-1)
    numerator = numerator * shrink[..., None] + jnp.einsum(
        "tgrs,sgd->tgrd",
        weights.astype(jnp.bfloat16),
        block_values,
        preferred_element_type=jnp.float32,
    )
    return (new_max, denominator, numerator)


def unchanged(carried):
    return carried


def collective_body(queries, keys_text, values_text, patch_rows, patch_owner, patch_place, value_head):
    token_count = queries.shape[1]
    kv_width = keys_text.shape[2]
    groups = kv_width // HD
    head_count = queries.shape[2] // HD
    group_size = head_count // groups
    score_scale = HD ** (-0.5)
    dp_count = lax.axis_size("dp")
    slot_count = dp_count * CAP
    owner_seq = patch_owner[0, 0, :, 0]
    places = patch_place[0, 0]
    owner_hits = (owner_seq[:, None] == jnp.arange(dp_count, dtype=jnp.int32)[None, :]).astype(
        jnp.int32
    )
    before = jnp.cumsum(owner_hits, axis=0) - owner_hits
    slot_rank = jnp.sum(before * owner_hits, axis=1)
    target = owner_seq * CAP + slot_rank
    select = (jnp.arange(slot_count, dtype=jnp.int32)[:, None] == target[None, :]).astype(jnp.int32)
    row_data = patch_rows[0, 0].reshape(places.shape[0], 2 * kv_width)
    packed = jnp.dot(
        select.astype(jnp.bfloat16), row_data, preferred_element_type=jnp.float32
    ).astype(jnp.bfloat16)
    filled = jnp.sum(select, axis=1)
    slot_place = jnp.sum(select * places[None, :], axis=1) + (1 - filled) * token_count
    packed = packed.reshape(slot_count, 2, kv_width)
    arrived, arrived_place = (
        lax.all_to_all(packed, "dp", split_axis=0, concat_axis=0, tiled=True),
        lax.all_to_all(slot_place, "dp", split_axis=0, concat_axis=0, tiled=True),
    )
    landing = (jnp.arange(token_count, dtype=jnp.int32)[:, None] == arrived_place[None, :]).astype(
        jnp.bfloat16
    )
    arrivals = jnp.dot(
        landing, arrived.reshape(slot_count, 2 * kv_width), preferred_element_type=jnp.float32
    )
    merged_keys = (keys_text[0].astype(jnp.float32) + arrivals[:, :kv_width]).astype(jnp.bfloat16)
    merged_values = (values_text[0].astype(jnp.float32) + arrivals[:, kv_width:]).astype(
        jnp.bfloat16
    )
    query_split = queries[0].reshape(token_count, groups, group_size, HD)
    first_row = lax.axis_index("ctx") * token_count
    query_place = first_row + jnp.arange(token_count, dtype=jnp.int32)
    initial = (
        jnp.full((token_count, groups, group_size), -1e30, jnp.float32),
        jnp.zeros((token_count, groups, group_size), jnp.float32),
        jnp.zeros((token_count, groups, group_size, HD), jnp.float32),
    )
    carried = initial
    start_row = jnp.int32(0)
    piece_keys = lax.all_gather(merged_keys, "ctx", axis=0, tiled=True)
    piece_values = lax.all_gather(merged_values, "ctx", axis=0, tiled=True)
    piece_rows = piece_keys.shape[0]
    block_rows = min(512, piece_rows)
    for lower in range(0, piece_rows, block_rows):
        upper = min(lower + block_rows, piece_rows)
        block_keys = piece_keys[lower:upper].reshape(upper - lower, groups, HD)
        block_values = piece_values[lower:upper].reshape(upper - lower, groups, HD)
        key_place = start_row + lower + jnp.arange(upper - lower, dtype=jnp.int32)

        def update(state_in):
            return attend_block(
                state_in, query_split, query_place, block_keys, block_values, key_place, score_scale
            )

        carried = lax.cond(
            start_row + lower <= first_row + token_count - 1, update, unchanged, carried
        )
    running_max, denominator, numerator = carried
    attention = (
        (numerator / denominator[..., None])
        .reshape(token_count, head_count * HD)
        .astype(jnp.bfloat16)
    )
    partial_value = jnp.dot(attention, value_head, preferred_element_type=jnp.float32)
    value_out = lax.psum(partial_value, "tp")
    return (attention[None], value_out[None])


def fused_kernel(
    dp_count,
    ctx_count,
    tp_count,
    owner_hbm,
    place_hbm,
    rows_hbm,
    keys_hbm,
    values_hbm,
    probe_hbm,
    queries_hbm,
    out_ref,
    value_ref,
    queries,
    text,
    rows_in,
    spots_in,
    merged_keys,
    merged_values,
    probe_raw,
    probe,
    partial,
    partial_in,
    query_sem,
    local_sem,
    text_send,
    text_recv,
    relay_send,
    patch_send,
    patch_recv,
    value_send,
    value_recv,
):
    d, c, t = lax.axis_index("dp"), lax.axis_index("ctx"), lax.axis_index("tp")
    token_count, kv_width = keys_hbm.shape
    groups = kv_width // HD
    heads = queries.shape[1] // HD
    group_size = heads // groups
    paired = ctx_count % 2 == 0
    side = lax.rem(c, 2)
    partner = c + 1 - 2 * side

    barrier = pltpu.get_barrier_semaphore()
    for k in range(dp_count):
        for m in range(ctx_count):
            if k or m:
                pl.semaphore_signal(
                    barrier,
                    inc=1,
                    device_id=(lax.rem(d + k, dp_count), lax.rem(c + m, ctx_count), t),
                    device_id_type=MESH,
                )
    for k in range(1, tp_count):
        pl.semaphore_signal(
            barrier, inc=1, device_id=(d, c, lax.rem(t + k, tp_count)), device_id_type=MESH
        )

    loads = [
        pltpu.make_async_copy(src, dst, local_sem.at[number])
        for number, (src, dst) in enumerate(
            (
                (rows_hbm, rows_in.at[c, d]),
                (owner_hbm, spots_in.at[c, d, 0]),
                (place_hbm, spots_in.at[c, d, 1]),
                (keys_hbm, text.at[c, 0]),
                (values_hbm, text.at[c, 1]),
                (probe_hbm, probe_raw),
            )
        )
    ]
    load_queries = pltpu.make_async_copy(queries_hbm, queries, query_sem)
    for load in loads:
        load.start()
    load_queries.start()
    for load in loads:
        load.wait()
    probe[...] = probe_raw[...].astype(jnp.float32)
    pl.semaphore_wait(barrier, dp_count * ctx_count - 1 + tp_count - 1)

    def patch_copies(k, later):
        there = lax.rem(d + k, dp_count)
        return [
            pltpu.make_async_remote_copy(
                src_ref=part.at[c, d],
                dst_ref=part.at[c, d],
                send_sem=patch_send.at[later, k, kind],
                recv_sem=patch_recv.at[c, d, kind],
                device_id=(there, later, t),
                device_id_type=MESH,
            )
            for kind, part in enumerate((rows_in, spots_in))
        ]

    def text_copies(later):
        return [
            pltpu.make_async_remote_copy(
                src_ref=text.at[c, kind],
                dst_ref=text.at[c, kind],
                send_sem=text_send.at[later, kind],
                recv_sem=text_recv.at[c, kind],
                device_id=(d, later, t),
                device_id_type=MESH,
            )
            for kind in range(2)
        ]

    def relay_copies(block):
        return [
            pltpu.make_async_remote_copy(
                src_ref=text.at[block, kind],
                dst_ref=text.at[block, kind],
                send_sem=relay_send.at[block, kind],
                recv_sem=text_recv.at[block, kind],
                device_id=(d, partner, t),
                device_id_type=MESH,
            )
            for kind in range(2)
        ]

    def sends_text(later):
        if not paired:
            return c < later
        return (c < later) & ((side == later % 2) | (partner == later))

    def for_patches(act):
        for k in range(dp_count):
            for later in range(ctx_count):
                reached = (c < later) if k == 0 else (c <= later)

                @pl.when(reached)
                def _():
                    for copy in patch_copies(k, later):
                        act(copy)

    def for_text(act):
        for later in range(1, ctx_count):

            @pl.when(sends_text(later))
            def _():
                for copy in text_copies(later):
                    act(copy)

    for_patches(lambda copy: copy.start())
    for_text(lambda copy: copy.start())

    def wait_text(block):
        for copy in relay_copies(block):
            copy.wait_recv()

    def wait_patches(block, first):
        for k in range(first, dp_count):
            there = lax.rem(d + k, dp_count)
            for kind, part in enumerate((rows_in, spots_in)):
                pltpu.make_async_remote_copy(
                    src_ref=part.at[block, there],
                    dst_ref=part.at[block, there],
                    send_sem=patch_send.at[0, k, kind],
                    recv_sem=patch_recv.at[block, there, kind],
                    device_id=(there, c, t),
                    device_id_type=MESH,
                ).wait_recv()

    def merge(block):
        slots = dp_count * rows_hbm.shape[0]
        spots = spots_in[block]
        code = spots[:, 0] * token_count + spots[:, 1]
        code = jnp.concatenate([code[k] for k in range(dp_count)], axis=1)
        here = d * token_count + lax.broadcasted_iota(jnp.int32, (token_count, slots), 0)
        landing = jnp.where(code == here, 1.0, 0.0).astype(jnp.bfloat16)
        rows = rows_in[block].astype(jnp.float32)
        row_keys = rows[:, :, 0, :].reshape(slots, kv_width).astype(jnp.bfloat16)
        row_values = rows[:, :, 1, :].reshape(slots, kv_width).astype(jnp.bfloat16)
        span = pl.ds(block * token_count, token_count)
        for kind, (rows, merged) in enumerate(
            ((row_keys, merged_keys), (row_values, merged_values))
        ):
            arrivals = jnp.dot(landing, rows, preferred_element_type=jnp.float32)
            merged[span, :] = (text[block, kind].astype(jnp.float32) + arrivals).astype(
                jnp.bfloat16
            )

    if paired:
        for block in range(ctx_count - 2):

            @pl.when((block < c) & (side == block % 2))
            def _():
                wait_text(block)

                @pl.when(block < c - side)
                def _():
                    for copy in relay_copies(block):
                        copy.start()

    for block in range(ctx_count):

        @pl.when(block == c)
        def _():
            wait_patches(block, 1)
            merge(block)

        @pl.when(block < c)
        def _():
            wait_patches(block, 0)
            if paired:

                @pl.when(side != block % 2)
                def _():
                    wait_text(block)

            else:
                wait_text(block)
            merge(block)

    load_queries.wait()
    score_scale = HD ** (-0.5) * math.log2(math.e)

    def attend(last):
        length = (last + 1) * token_count
        row = lax.broadcasted_iota(jnp.int32, (token_count, token_count), 0)
        col = lax.broadcasted_iota(jnp.int32, (token_count, token_count), 1)
        allowed = col <= row
        unroll = math.gcd(group_size, 4)

        def step(number, total):
            first = number * unroll
            lane = pl.multiple_of((first // group_size) * HD, HD)
            block_keys = merged_keys[0:length, pl.ds(lane, HD)]
            block_values = merged_values[0:length, pl.ds(lane, HD)]
            for extra in range(unroll):
                head = first + extra
                place = pl.ds(pl.multiple_of(head * HD, HD), HD)
                scores = lax.dot_general(
                    queries[:, place],
                    block_keys,
                    (((1,), (1,)), ((), ())),
                    preferred_element_type=jnp.float32,
                )
                parts = [
                    scores[:, j * token_count : (j + 1) * token_count] for j in range(last + 1)
                ]
                parts[last] = jnp.where(allowed, parts[last], -1e30)
                top = functools.reduce(jnp.maximum, parts)
                top = jnp.max(top, axis=1, keepdims=True)
                weights = [jnp.exp2((part - top) * score_scale) for part in parts]
                denominator = jnp.sum(
                    functools.reduce(jnp.add, weights), axis=1, keepdims=True
                )
                rounded = jnp.concatenate([w.astype(jnp.bfloat16) for w in weights], axis=1)
                numerator = jnp.dot(rounded, block_values, preferred_element_type=jnp.float32)
                result = (numerator * (1.0 / denominator)).astype(jnp.bfloat16)
                out_ref[:, place] = result
                total = total + result.astype(jnp.float32) * probe[pl.ds(head, 1), :]
            return total

        total = lax.fori_loop(
            0, heads // unroll, step, jnp.zeros((token_count, HD), jnp.float32)
        )
        partial[...] = jnp.sum(jnp.transpose(total), axis=0, keepdims=True)

    for last in range(ctx_count):

        @pl.when(c == last)
        def _():
            attend(last)

    value_copies = [
        pltpu.make_async_remote_copy(
            src_ref=partial,
            dst_ref=partial_in.at[k - 1],
            send_sem=value_send.at[k - 1],
            recv_sem=value_recv.at[k - 1],
            device_id=(d, c, lax.rem(t + k, tp_count)),
            device_id_type=MESH,
        )
        for k in range(1, tp_count)
    ]
    for copy in value_copies:
        copy.start()
    for_patches(lambda copy: copy.wait_send())
    for_text(lambda copy: copy.wait_send())
    if paired:
        for block in range(ctx_count - 2):

            @pl.when((block < c - side) & (side == block % 2))
            def _():
                for copy in relay_copies(block):
                    copy.wait_send()

    for copy in value_copies:
        copy.wait()
    whole = partial[...]
    for k in range(1, tp_count):
        whole = whole + partial_in[k - 1]
    value_ref[...] = whole


def fused_body(sizes, queries, keys_text, values_text, patch_rows, patch_owner, patch_place, value_head):
    dp_count, ctx_count, tp_count = sizes
    _, token_count, query_width = queries.shape
    kv_width = keys_text.shape[2]
    row_count = patch_rows.shape[2]
    heads = query_width // HD
    dma = pltpu.SemaphoreType.DMA
    vmem = pl.BlockSpec(memory_space=pltpu.VMEM)
    attention, value_out = pl.pallas_call(
        functools.partial(fused_kernel, dp_count, ctx_count, tp_count),
        out_shape=(
            jax.ShapeDtypeStruct((token_count, query_width), jnp.bfloat16),
            jax.ShapeDtypeStruct((1, token_count), jnp.float32),
        ),
        in_specs=[pl.BlockSpec(memory_space=pltpu.HBM)] * 7,
        out_specs=(vmem, vmem),
        scratch_shapes=[
            pltpu.VMEM((token_count, query_width), jnp.bfloat16),
            pltpu.VMEM((ctx_count, 2, token_count, kv_width), jnp.bfloat16),
            pltpu.VMEM((ctx_count, dp_count, row_count, 2, kv_width), jnp.bfloat16),
            pltpu.VMEM((ctx_count, dp_count, 2, 1, row_count), jnp.int32),
            pltpu.VMEM((ctx_count * token_count, kv_width), jnp.bfloat16),
            pltpu.VMEM((ctx_count * token_count, kv_width), jnp.bfloat16),
            pltpu.VMEM((heads, HD), jnp.bfloat16),
            pltpu.VMEM((heads, HD), jnp.float32),
            pltpu.VMEM((1, token_count), jnp.float32),
            pltpu.VMEM((max(tp_count - 1, 1), 1, token_count), jnp.float32),
            dma,
            dma((6,)),
            dma((ctx_count, 2)),
            dma((ctx_count, 2)),
            dma((ctx_count, 2)),
            dma((ctx_count, dp_count, 2)),
            dma((ctx_count, dp_count, 2)),
            dma((max(tp_count - 1, 1),)),
            dma((max(tp_count - 1, 1),)),
        ],
        compiler_params=pltpu.CompilerParams(
            collective_id=0, has_side_effects=True, vmem_limit_bytes=67043328
        ),
        name="merged_attention",
    )(
        patch_owner[0, 0].reshape(1, row_count),
        patch_place[0],
        patch_rows[0, 0],
        keys_text[0],
        values_text[0],
        value_head.reshape(heads, HD),
        queries[0],
    )
    return (attention[None], value_out)


def body(sizes, queries, keys_text, values_text, patch_rows, patch_owner, patch_place, value_head):
    dp_count, ctx_count, _ = sizes
    arriving = dp_count * ctx_count * patch_rows.size * patch_rows.dtype.itemsize
    arrays = (queries, keys_text, values_text, patch_rows, patch_owner, patch_place, value_head)
    if arriving > SLOT_BYTES:
        return collective_body(*arrays)
    return fused_body(sizes, *arrays)


def solution(mesh):
    in_specs = (
        P("dp", "ctx", "tp"),
        P("dp", "ctx", "tp"),
        P("dp", "ctx", "tp"),
        P("dp", "ctx", None, None, "tp"),
        P("dp", "ctx", None, None),
        P("dp", "ctx", None),
        P("tp"),
    )
    out_specs = (P("dp", "ctx", "tp"), P("dp", "ctx"))
    sizes = tuple(mesh.shape[axis] for axis in ("dp", "ctx", "tp"))
    return jax.shard_map(
        functools.partial(body, sizes),
        mesh=mesh,
        in_specs=in_specs,
        out_specs=out_specs,
        check_vma=False,
    )
```
